128 devices in a mesh: pts: 32 (over z, y_hi, x), orb: 4 (over y_lo, core).
Axes of the slice: x: 4, y: 4 (y_hi: 2, y_lo: 2; y = y_hi * 2 + y_lo), z: 4, core: 2. Of those that a mesh axis runs over, the one named last changes fastest.
Arguments:
- occ_points: float32 [20480, 1024], P('pts', 'orb'), may hold values from -0.1875 to 0.1875
- vir_points: float32 [20480, 9216], P('pts', 'orb'), may hold values from -0.0625 to 0.0625
- occ_cols: float32 [256, 1024], P('pts', 'orb'), may hold values from -6 to 6
- vir_cols: float32 [256, 9216], P('pts', 'orb'), may hold values from -6 to 6
- occ_energy: float32 [1024], P('orb'), may hold values from -1.5 to -0.2
- vir_energy: float32 [9216], P('orb'), may hold values from 0.2 to 3
- plane_waves: float32 [8192, 20480], P('orb', 'pts'), may hold values from -0.0390625 to 0.0390625
Outputs:
- projected: float32 [2, 8192, 256], P(None, 'orb', 'pts')
The draws below stay inside these ranges and needn't reach their ends.
All inputs are finite; a program needn't handle non-finite values.
Results may differ from the reference program's by a relative error of at most 0.00011.
Values sent between devices are 32-bit elements; how exact they have to be, the bound alone decides.
No kernel may reach another device: no remote copies, remote signals or barrier semaphores. Data moves between devices by JAX's collectives and lax.ppermute only.
A program may use at most 64 MiB of HBM per device.

```python
import jax
import jax.numpy as jnp
from jax import lax

NP = 20480
NOCC = 1024
NVIR = 9216
NPW = 8192
COLS = 256


def block_levels(stream_key, dims, cuts, low, high):
    def one(position, blocks):
        heights = jax.random.uniform(jax.random.fold_in(jax.random.fold_in(stream_key, 6), position), (blocks,), jnp.float32, low / len(cuts), high / len(cuts))
        return jnp.repeat(jnp.exp(heights), dims[position] // blocks).reshape((-1,) + (1,) * (len(dims) - position - 1))

    gain = one(*cuts[0])
    for cut in cuts[1:]:
        gain = gain * one(*cut)
    return gain


def normal_values(own_key, extent, spread, most, shards=(), dtype=jnp.bfloat16):
    values = spread * jax.random.normal(own_key, extent, jnp.float32)
    if shards:
        values = values * block_levels(own_key, extent, shards, -0.22, 0.18)
    return jnp.clip(values, -most, most).astype(dtype)


def setup_inputs(seed: int = 0) -> dict:
    streams_of = jax.random.split(jax.random.key(seed), 8)
    occ_points = normal_values(streams_of[0], (NP, NOCC), NOCC ** -0.5, 0.1875, ((0, 32), (1, 4)), jnp.float32)
    vir_points = normal_values(streams_of[1], (NP, NVIR), NVIR ** -0.5, 0.0625, ((0, 32), (1, 4)), jnp.float32)
    occ_cols = normal_values(streams_of[2], (COLS, NOCC), 1.0, 6.0, ((0, 32), (1, 4)), jnp.float32)
    vir_cols = normal_values(streams_of[3], (COLS, NVIR), 1.0, 6.0, ((0, 32), (1, 4)), jnp.float32)
    occ_energy = jnp.clip(-1.5 + 1.3 * jax.random.uniform(streams_of[4], (NOCC,), jnp.float32) ** block_levels(streams_of[4], (NOCC,), ((0, 4),), -0.2, 0.2), -1.5, -0.2)
    vir_energy = jnp.clip(0.2 + 2.8 * jax.random.uniform(streams_of[5], (NVIR,), jnp.float32) ** block_levels(streams_of[5], (NVIR,), ((0, 4),), -0.2, 0.2), 0.2, 3.0)
    plane_waves = normal_values(streams_of[6], (NPW, NP), NP ** -0.5, 0.0390625, ((0, 4), (1, 32)), jnp.float32)
    return {"occ_points": occ_points, "vir_points": vir_points, "occ_cols": occ_cols, "vir_cols": vir_cols, "occ_energy": occ_energy, "vir_energy": vir_energy, "plane_waves": plane_waves}


IMAG_TIMES = (0.3, 1.2)
FREQUENCIES = (0.5, 2.0)
QUAD_WEIGHTS = (0.6, 1.8)


def make_table():
    moments = jnp.array(IMAG_TIMES, jnp.float32)
    omegas = jnp.array(FREQUENCIES, jnp.float32)
    weights = jnp.array(QUAD_WEIGHTS, jnp.float32)
    return 2.0 * weights[None, :] * jnp.cos(omegas[:, None] * moments[None, :])


def contract(left, right):
    return lax.dot_general(left, right, (((1,), (1,)), ((), ())), precision=lax.Precision.HIGHEST, preferred_element_type=jnp.float32)


def reference(occ_points, vir_points, occ_cols, vir_cols, occ_energy, vir_energy, plane_waves):
    moments = jnp.array(IMAG_TIMES, jnp.float32)
    occ_weight = jnp.exp(moments[:, None] * occ_energy[None, :])
    vir_weight = jnp.exp(-moments[:, None] * vir_energy[None, :])
    point_count = occ_points.shape[0]
    columns = occ_cols.shape[0]
    occ_scaled = (occ_cols[None, :, :] * occ_weight[:, None, :]).reshape(2 * columns, -1)
    vir_scaled = (vir_cols[None, :, :] * vir_weight[:, None, :]).reshape(2 * columns, -1)
    occ_green = contract(occ_points, occ_scaled).reshape(point_count, 2, columns)
    vir_green = contract(vir_points, vir_scaled).reshape(point_count, 2, columns)
    response = -(occ_green * vir_green)
    spectral = jnp.einsum('kt,rtc->rkc', make_table(), response, precision=lax.Precision.HIGHEST)
    partial_value = jnp.dot(plane_waves, spectral.reshape(point_count, 2 * columns), precision=lax.Precision.HIGHEST, preferred_element_type=jnp.float32)
    return jnp.transpose(partial_value.reshape(plane_waves.shape[0], 2, columns), (1, 0, 2))
```

```python
import math

import jax
import jax.numpy as jnp
from jax import lax
from jax.experimental import pallas as pl
from jax.experimental.pallas import tpu as pltpu
from jax.sharding import Mesh
from jax.sharding import PartitionSpec as P

PTS = ("z", "yh", "x")
ORB = ("yl", "core")
SIDE = 4

IMAG_TIMES = (0.3, 1.2)
FREQUENCIES = (0.5, 2.0)
QUAD_WEIGHTS = (0.6, 1.8)
TABLE = [[2.0 * q * math.cos(w * t) for q, t in zip(QUAD_WEIGHTS, IMAG_TIMES)] for w in FREQUENCIES]

VMEM_LIMIT = 50 * 1024 * 1024


def swap(x, axis):
    return lax.ppermute(x, axis, [(0, 1), (1, 0)])


def outer_shift(x, by):
    pairs = []
    for z in range(SIDE):
        for k in range(SIDE):
            for core in range(2):
                to = (z, (k + by) % SIDE) if core else ((z + by) % SIDE, k)
                pairs.append(((z * SIDE + k) * 2 + core, (to[0] * SIDE + to[1]) * 2 + core))
    return lax.ppermute(x, ("z", "x", "core"), pairs)


def inner_pairs(by, other):
    place = lambda z, y, x, c: (((z % SIDE) * 2 + y) * SIDE + x % SIDE) * 2 + c
    pairs = []
    for z in range(SIDE):
        for y in range(2):
            for x in range(SIDE):
                near = place(z, y, x + by, 1 if other else 0)
                far = place(z + by, 1 - y, x, 0 if other else 1)
                pairs += [(place(z, y, x, 0), near), (place(z, y, x, 1), far)]
    return pairs


def to_owner(x, by, other):
    return lax.ppermute(x, PTS + ("core",), inner_pairs(by, other))


def from_owner(x, by, other):
    pairs = [(b, a) for a, b in inner_pairs(by, other)]
    return lax.ppermute(x, PTS + ("core",), pairs)


def joined(blocks):
    rows, width = blocks[0].shape
    n = len(blocks) // 2

    def body(*refs):
        for i in range(n):
            for s in range(2):
                at = (pl.ds(i * rows, rows), pl.ds(s * width, width))
                refs[2 * n][at] = refs[2 * i + s][...]

    return pl.pallas_call(
        body,
        out_shape=jax.ShapeDtypeStruct((n * rows, 2 * width), blocks[0].dtype),
        name="joined",
    )(*blocks)


def picked(blocks, energy, occ_count, core_width):
    rows = blocks[0].shape[0]
    n = len(blocks)

    def body(*refs):
        ins, last, out = refs[: 2 * n], refs[2 * n], refs[2 * n + 1]
        for i in range(n):
            for s in range(2):
                at = (pl.ds(i * rows, rows), pl.ds(s * occ_count, occ_count))
                out[at] = ins[2 * i + s][...]
        out[pl.ds(n * rows, 8), :] = last[...]

    def slot(s):
        at = s * core_width // occ_count
        return pl.BlockSpec((rows, occ_count), lambda i: (0, at))

    return pl.pallas_call(
        body,
        grid=(1,),
        in_specs=[slot(s) for _ in range(n) for s in range(2)]
        + [pl.BlockSpec(energy.shape, lambda i: (0, 0))],
        out_specs=pl.BlockSpec((n * rows + 8, 2 * occ_count), lambda i: (0, 0)),
        out_shape=jax.ShapeDtypeStruct((n * rows + 8, 2 * occ_count), blocks[0].dtype),
        name="picked",
    )(*[b for b in blocks for _ in range(2)], energy)


def parts(x):
    high = lax.reduce_precision(x, 8, 7)
    return high.astype(jnp.bfloat16), (x - high).astype(jnp.bfloat16)


def parts_in_kernel(x):
    high = x.astype(jnp.bfloat16)
    return high, (x - high.astype(jnp.float32)).astype(jnp.bfloat16)


def contract(left, right):
    return lax.dot_general(
        left, right, (((1,), (1,)), ((), ())), preferred_element_type=jnp.float32
    )


def contract_parts(left, right):
    return (
        contract(left[0], right[0]) + contract(left[0], right[1]) + contract(left[1], right[0])
    )


def vir_greens(blocks, weight, point_sets, occ_count):
    n = len(blocks)
    rows = blocks[0].shape[0]
    half = blocks[0].shape[1] // 2
    width = half - occ_count
    points = point_sets[0].shape[0]
    step = 768 if width % 768 == 0 else width
    per = width // step

    def body(*refs):
        ins, w_ref = refs[:n], refs[n]
        sets = refs[n + 1 : n + 3]
        out, total, high, low = refs[n + 3 :]
        i = pl.program_id(0)

        for s in range(2):

            @pl.when(i // per == s)
            def _(s=s):
                k = pl.multiple_of((i - s * per) * step, 128)
                w = w_ref[:, pl.ds(s * width + k, step)]
                for j in range(n):
                    x = ins[j][:, pl.ds(s * half + occ_count + k, step)]
                    for t in range(2):
                        at = pl.ds((t * n + j) * rows, rows)
                        high[at, :], low[at, :] = parts_in_kernel(x * w[t : t + 1])
                part = contract_parts(parts_in_kernel(sets[s][...]), (high[...], low[...]))
                if s == 0:

                    @pl.when(i == 0)
                    def _():
                        total[...] = part

                    @pl.when(i > 0)
                    def _():
                        total[...] += part

                else:
                    total[...] += part

        @pl.when(i == 2 * per - 1)
        def _():
            out[...] = total[...].T

    whole = lambda a: pl.BlockSpec(a.shape, lambda i: (0, 0))
    return pl.pallas_call(
        body,
        grid=(2 * per,),
        in_specs=[whole(b) for b in blocks]
        + [whole(weight)]
        + [
            pl.BlockSpec((points, step), lambda i: (0, jnp.minimum(i, per - 1))),
            pl.BlockSpec((points, step), lambda i: (0, jnp.maximum(i - per, 0))),
        ],
        out_specs=pl.BlockSpec((2 * n * rows, points), lambda i: (0, 0)),
        out_shape=jax.ShapeDtypeStruct((2 * n * rows, points), jnp.float32),
        scratch_shapes=[pltpu.VMEM((points, 2 * n * rows), jnp.float32)]
        + [pltpu.VMEM((2 * n * rows, step), jnp.bfloat16)] * 2,
        compiler_params=pltpu.CompilerParams(vmem_limit_bytes=VMEM_LIMIT),
        cost_estimate=pl.CostEstimate(
            flops=12 * n * rows * points * 2 * width, bytes_accessed=20_000_000, transcendentals=0
        ),
        name="vir_greens",
    )(*blocks, weight, *point_sets)


def projections(vir_here, vir_there, occ, wave_parts, own):
    rows, points = occ.shape
    waves = wave_parts[0].shape[0]
    step = 512
    share = rows // SIDE

    def body(a_ref, b_ref, o_ref, w_high, w_low, *refs):
        outs, (high, low) = refs[:SIDE], refs[SIDE:]

        @pl.when(pl.program_id(0) == 0)
        def _():
            response = -(o_ref[...] * (a_ref[...] + b_ref[...]))
            early, late = response[: rows // 2], response[rows // 2 :]
            spectral = [TABLE[k][0] * early + TABLE[k][1] * late for k in range(2)]
            for i in range(rows // (2 * own)):
                block = jnp.concatenate([s[i * own : (i + 1) * own] for s in spectral], axis=0)
                at = pl.ds(2 * own * i, 2 * own)
                high[at, :], low[at, :] = parts_in_kernel(block)

        result = contract_parts((high[...], low[...]), (w_high[...], w_low[...]))
        for d in range(SIDE):
            outs[d][...] = result[d * share : (d + 1) * share]

    whole = pl.BlockSpec((rows, points), lambda i: (0, 0))
    return pl.pallas_call(
        body,
        grid=(waves // step,),
        in_specs=[whole] * 3 + [pl.BlockSpec((step, points), lambda i: (i, 0))] * 2,
        out_specs=[pl.BlockSpec((share, step), lambda i: (0, i))] * SIDE,
        out_shape=[jax.ShapeDtypeStruct((share, waves), jnp.float32)] * SIDE,
        scratch_shapes=[pltpu.VMEM((rows, points), jnp.bfloat16)] * 2,
        compiler_params=pltpu.CompilerParams(vmem_limit_bytes=VMEM_LIMIT),
        cost_estimate=pl.CostEstimate(
            flops=6 * rows * points * waves, bytes_accessed=8_000_000, transcendentals=0
        ),
        name="projections",
    )(vir_here, vir_there, occ, *wave_parts)


def summed_blocks(arrays):
    rows, waves = arrays[0].shape
    step = 1024
    share = rows // SIDE

    def body(*refs):
        total = refs[0][...]
        for r in refs[1:SIDE]:
            total = total + r[...]
        for d in range(SIDE):
            refs[SIDE + d][...] = total[d * share : (d + 1) * share]

    return pl.pallas_call(
        body,
        grid=(waves // step,),
        in_specs=[pl.BlockSpec((rows, step), lambda i: (0, i))] * SIDE,
        out_specs=[pl.BlockSpec((share, step), lambda i: (0, i))] * SIDE,
        out_shape=[jax.ShapeDtypeStruct((share, waves), jnp.float32)] * SIDE,
        cost_estimate=pl.CostEstimate(
            flops=3 * rows * waves, bytes_accessed=20 * rows * waves, transcendentals=0
        ),
        name="summed_blocks",
    )(*arrays)


def on_device(occ_points, vir_points, occ_cols, vir_cols, occ_energy, vir_energy, plane_waves):
    points, occ_count = occ_points.shape
    own = occ_cols.shape[0]
    moments = jnp.array(IMAG_TIMES, jnp.float32)

    cols = jnp.concatenate([occ_cols, vir_cols], axis=1)
    block = joined([from_owner(cols, d, other) for d in range(SIDE) for other in (False, True)])
    blocks = [block] + [outer_shift(block, -d) for d in range(1, SIDE)]

    energy = jnp.concatenate([occ_energy, vir_energy])
    energy_other = swap(energy, "core")
    vir_both = jnp.concatenate([vir_energy, energy_other[occ_count:]])
    vir_weight = jnp.exp(-moments[:, None] * vir_both[None, :])
    occ_chip = jnp.concatenate([occ_energy, energy_other[:occ_count]])
    occ_chip = jnp.broadcast_to(occ_chip[None], (8, 2 * occ_count))
    occ_here = picked(blocks, occ_chip, occ_count, cols.shape[1])
    occ_there = swap(occ_here, "yl")
    vir_green = vir_greens(blocks, vir_weight, (vir_points, swap(vir_points, "core")), occ_count)

    vir_there = swap(vir_green, "yl")
    occ_sets = [occ_points, swap(occ_points, "yl")]
    occ_sets = [occ_sets[0], swap(occ_sets[0], "core"), occ_sets[1], swap(occ_sets[1], "core")]
    waves = [swap(plane_waves, "core"), plane_waves]
    vir_green, occ_here, occ_there, occ_sets, waves = lax.optimization_barrier(
        (vir_green, occ_here, occ_there, occ_sets, waves)
    )
    occ_both = jnp.concatenate([occ_here, occ_there], axis=1)
    columns = occ_here.shape[0] - 8
    occ_weight = jnp.exp(moments[:, None] * occ_both[columns][None, :])
    occ_scaled = occ_both[None, :columns, :] * occ_weight[:, None, :]
    occ_scaled = occ_scaled.reshape(2 * columns, -1)
    occ_green = contract_parts(parts(occ_scaled), parts(jnp.concatenate(occ_sets, axis=1)))
    waves = [parts(w) for w in waves]

    results = []
    for w, other in zip(waves, (True, False)):
        sums = projections(vir_green, vir_there, occ_green, w, own)
        sums = [sums[0]] + [outer_shift(sums[d], d) for d in range(1, SIDE)]
        sums = summed_blocks(sums)
        results += [to_owner(sums[d], d, other) for d in range(SIDE)]
    total = sum(results[1:], results[0])
    return jnp.transpose(total.reshape(2, own, -1), (0, 2, 1))


def solution(mesh):
    split = Mesh(mesh.devices.reshape(SIDE, 2, SIDE, 2, 2), PTS + ORB)
    in_specs = (
        P(PTS, ORB),
        P(PTS, ORB),
        P(PTS, ORB),
        P(PTS, ORB),
        P(ORB),
        P(ORB),
        P(ORB, PTS),
    )
    out_specs = P(None, ORB, PTS)
    return jax.shard_map(
        on_device, mesh=split, in_specs=in_specs, out_specs=out_specs, check_vma=False
    )
```

```python
import math

import jax
import jax.numpy as jnp
from jax import lax
from jax.experimental import pallas as pl
from jax.experimental.pallas import tpu as pltpu
from jax.sharding import Mesh
from jax.sharding import PartitionSpec as P

PTS = ("z", "yh", "x")
ORB = ("yl", "core")
SIDE = 4

IMAG_TIMES = (0.3, 1.2)
FREQUENCIES = (0.5, 2.0)
QUAD_WEIGHTS = (0.6, 1.8)
TABLE = [[2.0 * q * math.cos(w * t) for q, t in zip(QUAD_WEIGHTS, IMAG_TIMES)] for w in FREQUENCIES]

MIB = 1024 * 1024


def limit(mib):
    return pltpu.CompilerParams(vmem_limit_bytes=mib * MIB)


def swap(x, axis):
    return lax.ppermute(x, axis, [(0, 1), (1, 0)])


def outer_shift(x, by):
    pairs = []
    for z in range(SIDE):
        for k in range(SIDE):
            for core in range(2):
                to = (z, (k + by) % SIDE) if core else ((z + by) % SIDE, k)
                pairs.append(((z * SIDE + k) * 2 + core, (to[0] * SIDE + to[1]) * 2 + core))
    return lax.ppermute(x, ("z", "x", "core"), pairs)


def inner_shift(x, by):
    pairs = []
    for z in range(SIDE):
        for k in range(SIDE):
            for core in range(2):
                to = ((z + by) % SIDE, k) if core else (z, (k + by) % SIDE)
                pairs.append(((z * SIDE + k) * 2 + core, (to[0] * SIDE + to[1]) * 2 + core))
    return lax.ppermute(x, ("z", "x", "core"), pairs)


def inner_pairs(by, other):
    place = lambda z, y, x, c: (((z % SIDE) * 2 + y) * SIDE + x % SIDE) * 2 + c
    pairs = []
    for z in range(SIDE):
        for y in range(2):
            for x in range(SIDE):
                near = place(z, y, x + by, 1 if other else 0)
                far = place(z + by, 1 - y, x, 0 if other else 1)
                pairs += [(place(z, y, x, 0), near), (place(z, y, x, 1), far)]
    return pairs


def to_owner(x, by, other):
    return lax.ppermute(x, PTS + ("core",), inner_pairs(by, other))


def from_owner(x, by, other):
    pairs = [(b, a) for a, b in inner_pairs(by, other)]
    return lax.ppermute(x, PTS + ("core",), pairs)


def joined(blocks, axis):
    shape = list(blocks[0].shape)
    shape[axis] = sum(b.shape[axis] for b in blocks)

    def body(*refs):
        start = 0
        for r in refs[:-1]:
            at = pl.ds(start, r.shape[axis])
            if axis:
                refs[-1][:, at] = r[...]
            else:
                refs[-1][at, :] = r[...]
            start += r.shape[axis]

    return pl.pallas_call(
        body,
        out_shape=jax.ShapeDtypeStruct(tuple(shape), blocks[0].dtype),
        compiler_params=limit(6),
        name="joined",
    )(*blocks)


def picked(blocks, energy, occ_count, core_width):
    rows = blocks[0].shape[0]
    n = len(blocks)

    def body(*refs):
        ins, last, out = refs[: 2 * n], refs[2 * n], refs[2 * n + 1]
        for i in range(n):
            for s in range(2):
                at = (pl.ds(i * rows, rows), pl.ds(s * occ_count, occ_count))
                out[at] = ins[2 * i + s][...]
        out[pl.ds(n * rows, 8), :] = last[...]

    def slot(s):
        at = s * core_width // occ_count
        return pl.BlockSpec((rows, occ_count), lambda i: (0, at))

    return pl.pallas_call(
        body,
        grid=(1,),
        in_specs=[slot(s) for _ in range(n) for s in range(2)]
        + [pl.BlockSpec(energy.shape, lambda i: (0, 0))],
        out_specs=pl.BlockSpec((n * rows + 8, 2 * occ_count), lambda i: (0, 0)),
        out_shape=jax.ShapeDtypeStruct((n * rows + 8, 2 * occ_count), blocks[0].dtype),
        compiler_params=limit(4),
        name="picked",
    )(*[b for b in blocks for _ in range(2)], energy)


def parts(x):
    high = x.astype(jnp.bfloat16)
    return high, (x - high.astype(jnp.float32)).astype(jnp.bfloat16)


def contract(left, right):
    return lax.dot_general(
        left, right, (((1,), (1,)), ((), ())), preferred_element_type=jnp.float32
    )


def contract_parts(stacked, right):
    rows = stacked.shape[0] // 2
    high, low = parts(right)
    both = contract(stacked, high)
    return (both[:rows] + both[rows:]) + contract(stacked[:rows], low)


def vir_greens(blocks, weight, point_sets, occ_count):
    n = len(blocks)
    rows = blocks[0].shape[0]
    half = blocks[0].shape[1] // 2
    width = half - occ_count
    points = point_sets[0].shape[0]
    step = 768 if width % 768 == 0 else width
    per = width // step
    total = 2 * n * rows

    def body(*refs):
        ins, w_ref = refs[:n], refs[n]
        sets = refs[n + 1 : n + 3]
        out, stacked = refs[n + 3 :]
        i = pl.program_id(0)

        @pl.when(i == 0)
        def _():
            out[...] = jnp.zeros_like(out)

        for s in range(2):

            @pl.when(i // per == s)
            def _(s=s):
                k = pl.multiple_of((i - s * per) * step, 128)
                w = w_ref[:, pl.ds(s * width + k, step)]
                for j in range(n):
                    x = ins[j][:, pl.ds(s * half + occ_count + k, step)]
                    for t in range(2):
                        at = (t * n + j) * rows
                        high, low = parts(x * w[t : t + 1])
                        stacked[pl.ds(at, rows), :] = high
                        stacked[pl.ds(total + at, rows), :] = low
                out[...] += contract_parts(stacked[...], sets[s][...])

    whole = lambda a: pl.BlockSpec(a.shape, lambda i: (0, 0))
    return pl.pallas_call(
        body,
        grid=(2 * per,),
        in_specs=[whole(b) for b in blocks]
        + [whole(weight)]
        + [
            pl.BlockSpec((points, step), lambda i: (0, jnp.minimum(i, per - 1))),
            pl.BlockSpec((points, step), lambda i: (0, jnp.maximum(i - per, 0))),
        ],
        out_specs=pl.BlockSpec((total, points), lambda i: (0, 0)),
        out_shape=jax.ShapeDtypeStruct((total, points), jnp.float32),
        scratch_shapes=[pltpu.VMEM((2 * total, step), jnp.bfloat16)],
        compiler_params=limit(24),
        cost_estimate=pl.CostEstimate(
            flops=6 * total * points * 2 * width, bytes_accessed=14_000_000, transcendentals=0
        ),
        name="vir_greens",
    )(*blocks, weight, *point_sets)


def occ_greens(here, there, point_sets):
    columns = here.shape[0] - 8
    width = here.shape[1]
    points, count = point_sets[0].shape

    def body(here_ref, there_ref, *refs):
        sets, (out, stacked) = refs[:4], refs[4:]
        total = None
        for chip, ref in enumerate((here_ref, there_ref)):
            energy = ref[pl.ds(columns, 1), :]
            for t in range(2):
                x = ref[pl.ds(0, columns), :] * jnp.exp(IMAG_TIMES[t] * energy)
                high, low = parts(x)
                k = pl.ds(chip * width, width)
                stacked[pl.ds(t * columns, columns), k] = high
                stacked[pl.ds((2 + t) * columns, columns), k] = low
        for i in range(4):
            part = contract_parts(stacked[:, pl.ds(i * count, count)], sets[i][...])
            total = part if total is None else total + part
        out[...] = total

    return pl.pallas_call(
        body,
        out_shape=jax.ShapeDtypeStruct((2 * columns, points), jnp.float32),
        scratch_shapes=[pltpu.VMEM((4 * columns, 2 * width), jnp.bfloat16)],
        compiler_params=limit(16),
        name="occ_greens",
    )(here, there, *point_sets)


def projections(vir_here, vir_there, occ, wave_sets, own):
    rows, points = occ.shape
    waves = wave_sets[0].shape[0]
    step = 512
    per = waves // step
    blocks = rows // (2 * own * SIDE)
    share = rows // blocks
    inner = share // (2 * own)

    def body(a_ref, b_ref, o_ref, w_first, w_last, *refs):
        outs, stacked = refs[:-1], refs[-1]
        i = pl.program_id(0)

        @pl.when(i == 0)
        def _():
            response = -(o_ref[...] * (a_ref[...] + b_ref[...]))
            early, late = response[: rows // 2], response[rows // 2 :]
            spectral = [TABLE[k][0] * early + TABLE[k][1] * late for k in range(2)]
            for j in range(blocks * inner):
                both = jnp.concatenate([s[j * own : (j + 1) * own] for s in spectral], axis=0)
                high, low = parts(both)
                stacked[pl.ds(2 * own * j, 2 * own), :] = high
                stacked[pl.ds(rows + 2 * own * j, 2 * own), :] = low

        for s, w_ref in enumerate((w_first, w_last)):

            @pl.when(i // per == s)
            def _(s=s, w_ref=w_ref):
                result = contract_parts(stacked[...], w_ref[...])
                for d in range(blocks):
                    outs[s * blocks + d][...] = result[d * share : (d + 1) * share]

    whole = pl.BlockSpec((rows, points), lambda i: (0, 0))
    first = lambda i: jnp.minimum(i, per - 1)
    last = lambda i: jnp.maximum(i - per, 0)
    return pl.pallas_call(
        body,
        grid=(2 * per,),
        in_specs=[whole] * 3
        + [
            pl.BlockSpec((step, points), lambda i: (first(i), 0)),
            pl.BlockSpec((step, points), lambda i: (last(i), 0)),
        ],
        out_specs=[pl.BlockSpec((share, step), lambda i: (0, first(i)))] * blocks
        + [pl.BlockSpec((share, step), lambda i: (0, last(i)))] * blocks,
        out_shape=[jax.ShapeDtypeStruct((share, waves), jnp.float32)] * (2 * blocks),
        scratch_shapes=[pltpu.VMEM((2 * rows, points), jnp.bfloat16)],
        compiler_params=limit(24),
        cost_estimate=pl.CostEstimate(
            flops=12 * rows * points * waves, bytes_accessed=14_000_000, transcendentals=0
        ),
        name="projections",
    )(vir_here, vir_there, occ, *wave_sets)


def summed_blocks(arrays):
    rows, waves = arrays[0].shape
    step = 1024
    share = rows // SIDE

    def body(*refs):
        total = refs[0][...]
        for r in refs[1:SIDE]:
            total = total + r[...]
        for d in range(SIDE):
            refs[SIDE + d][...] = total[d * share : (d + 1) * share]

    return pl.pallas_call(
        body,
        grid=(waves // step,),
        in_specs=[pl.BlockSpec((rows, step), lambda i: (0, i))] * SIDE,
        out_specs=[pl.BlockSpec((share, step), lambda i: (0, i))] * SIDE,
        out_shape=[jax.ShapeDtypeStruct((share, waves), jnp.float32)] * SIDE,
        compiler_params=limit(12),
        cost_estimate=pl.CostEstimate(
            flops=3 * rows * waves, bytes_accessed=20 * rows * waves, transcendentals=0
        ),
        name="summed_blocks",
    )(*arrays)


def after(x, event):
    return lax.optimization_barrier((x, event))[0]


def on_device(occ_points, vir_points, occ_cols, vir_cols, occ_energy, vir_energy, plane_waves):
    _, occ_count = occ_points.shape
    own = occ_cols.shape[0]
    moments = jnp.array(IMAG_TIMES, jnp.float32)

    cols = joined([occ_cols, vir_cols], 1)
    block = joined([from_owner(cols, 0, other) for other in (False, True)], 1)
    occ_points_there = swap(after(occ_points, block), "yl")
    block = joined([block] + [inner_shift(block, -d) for d in range(1, SIDE)], 0)
    blocks = [block] + [None] * (SIDE - 1)
    for d in (1, 3, 2):
        blocks[d] = outer_shift(block, -d)

    energy = jnp.concatenate([occ_energy, vir_energy])
    energy_other = swap(energy, "core")
    vir_both = jnp.concatenate([vir_energy, energy_other[occ_count:]])
    vir_weight = jnp.exp(-moments[:, None] * vir_both[None, :])
    occ_chip = jnp.concatenate([occ_energy, energy_other[:occ_count]])
    occ_chip = jnp.broadcast_to(occ_chip[None], (8, 2 * occ_count))
    vir_sets = (vir_points, swap(vir_points, "core"))
    occ_sets = None

    sums = [[None] * SIDE for _ in range(2)]
    for group in ((1, 3), (0, 2)):
        pair = [blocks[d] for d in group]
        occ_here = picked(pair, occ_chip, occ_count, cols.shape[1])
        occ_there = swap(occ_here, "yl")
        vir_here = vir_greens(pair, vir_weight, vir_sets, occ_count)
        vir_there = swap(vir_here, "yl")
        if occ_sets is None:
            near, far, waves = after((occ_points, occ_points_there, plane_waves), vir_here)
            occ_sets = (near, swap(near, "core"), far, swap(far, "core"))
            wave_sets = (plane_waves, swap(waves, "core"))
        occ_green = occ_greens(occ_here, occ_there, occ_sets)
        found = projections(vir_here, vir_there, occ_green, wave_sets, own)
        for s in range(2):
            for j, d in enumerate(group):
                sums[s][d] = outer_shift(found[2 * s + j], d) if d else found[2 * s + j]

    results = []
    for s, other in enumerate((False, True)):
        finished = summed_blocks(sums[s])
        results += [to_owner(finished[d], d, other) for d in range(SIDE)]
    total = sum(results[1:], results[0])
    return jnp.transpose(total.reshape(2, own, -1), (0, 2, 1))


def solution(mesh):
    split = Mesh(mesh.devices.reshape(SIDE, 2, SIDE, 2, 2), PTS + ORB)
    in_specs = (
        P(PTS, ORB),
        P(PTS, ORB),
        P(PTS, ORB),
        P(PTS, ORB),
        P(ORB),
        P(ORB),
        P(ORB, PTS),
    )
    out_specs = P(None, ORB, PTS)
    return jax.shard_map(
        on_device, mesh=split, in_specs=in_specs, out_specs=out_specs, check_vma=False
    )
```

```python
import math

import jax
import jax.numpy as jnp
from jax import lax
from jax.experimental import pallas as pl
from jax.experimental.pallas import tpu as pltpu
from jax.sharding import Mesh
from jax.sharding import PartitionSpec as P

PTS = ("z", "yh", "x")
ORB = ("yl", "core")
SIDE = 4

IMAG_TIMES = (0.3, 1.2)
FREQUENCIES = (0.5, 2.0)
QUAD_WEIGHTS = (0.6, 1.8)
TABLE = [[2.0 * q * math.cos(w * t) for q, t in zip(QUAD_WEIGHTS, IMAG_TIMES)] for w in FREQUENCIES]

MIB = 1024 * 1024


def limit(mib):
    return pltpu.CompilerParams(vmem_limit_bytes=mib * MIB)


def swap(x, axis):
    return lax.ppermute(x, axis, [(0, 1), (1, 0)])


def outer_shift(x, by):
    pairs = []
    for z in range(SIDE):
        for k in range(SIDE):
            for core in range(2):
                to = (z, (k + by) % SIDE) if core else ((z + by) % SIDE, k)
                pairs.append(((z * SIDE + k) * 2 + core, (to[0] * SIDE + to[1]) * 2 + core))
    return lax.ppermute(x, ("z", "x", "core"), pairs)


def inner_shift(x, by):
    pairs = []
    for z in range(SIDE):
        for k in range(SIDE):
            for core in range(2):
                to = ((z + by) % SIDE, k) if core else (z, (k + by) % SIDE)
                pairs.append(((z * SIDE + k) * 2 + core, (to[0] * SIDE + to[1]) * 2 + core))
    return lax.ppermute(x, ("z", "x", "core"), pairs)


def inner_pairs(by, other):
    place = lambda z, y, x, c: (((z % SIDE) * 2 + y) * SIDE + x % SIDE) * 2 + c
    pairs = []
    for z in range(SIDE):
        for y in range(2):
            for x in range(SIDE):
                near = place(z, y, x + by, 1 if other else 0)
                far = place(z + by, 1 - y, x, 0 if other else 1)
                pairs += [(place(z, y, x, 0), near), (place(z, y, x, 1), far)]
    return pairs


def to_owner(x, by, other):
    return lax.ppermute(x, PTS + ("core",), inner_pairs(by, other))


def from_owner(x, by, other):
    pairs = [(b, a) for a, b in inner_pairs(by, other)]
    return lax.ppermute(x, PTS + ("core",), pairs)


def joined(blocks, axis):
    shape = list(blocks[0].shape)
    shape[axis] = sum(b.shape[axis] for b in blocks)

    def body(*refs):
        start = 0
        for r in refs[:-1]:
            at = pl.ds(start, r.shape[axis])
            if axis:
                refs[-1][:, at] = r[...]
            else:
                refs[-1][at, :] = r[...]
            start += r.shape[axis]

    return pl.pallas_call(
        body,
        out_shape=jax.ShapeDtypeStruct(tuple(shape), blocks[0].dtype),
        compiler_params=limit(6),
        name="joined",
    )(*blocks)


def picked(blocks, energy, occ_count, core_width):
    rows = blocks[0].shape[0]
    n = len(blocks)

    def body(*refs):
        ins, last, out = refs[: 2 * n], refs[2 * n], refs[2 * n + 1]
        for i in range(n):
            for s in range(2):
                at = (pl.ds(i * rows, rows), pl.ds(s * occ_count, occ_count))
                out[at] = ins[2 * i + s][...]
        out[pl.ds(n * rows, 8), :] = last[...]

    def slot(s):
        at = s * core_width // occ_count
        return pl.BlockSpec((rows, occ_count), lambda i: (0, at))

    return pl.pallas_call(
        body,
        grid=(1,),
        in_specs=[slot(s) for _ in range(n) for s in range(2)]
        + [pl.BlockSpec(energy.shape, lambda i: (0, 0))],
        out_specs=pl.BlockSpec((n * rows + 8, 2 * occ_count), lambda i: (0, 0)),
        out_shape=jax.ShapeDtypeStruct((n * rows + 8, 2 * occ_count), blocks[0].dtype),
        compiler_params=limit(4),
        name="picked",
    )(*[b for b in blocks for _ in range(2)], energy)


def parts(x):
    high = x.astype(jnp.bfloat16)
    return high, (x - high.astype(jnp.float32)).astype(jnp.bfloat16)


def contract(left, right):
    return lax.dot_general(
        left, right, (((1,), (1,)), ((), ())), preferred_element_type=jnp.float32
    )


def split(x):
    rows, width = x.shape
    step = 768 if width % 768 == 0 else width

    def body(ref, high, low):
        high[...], low[...] = parts(ref[...])

    spec = pl.BlockSpec((rows, step), lambda i: (0, i))
    return pl.pallas_call(
        body,
        grid=(width // step,),
        in_specs=[spec],
        out_specs=[spec] * 2,
        out_shape=[jax.ShapeDtypeStruct(x.shape, jnp.bfloat16)] * 2,
        compiler_params=limit(12),
        name="split",
    )(x)


def contract_parts(stacked, high, low):
    rows = stacked.shape[0] // 2
    both = contract(stacked, high)
    return (both[:rows] + both[rows:]) + contract(stacked[:rows], low)


def vir_greens(blocks, weight, point_sets, occ_count):
    n = len(blocks)
    rows = blocks[0].shape[0]
    half = blocks[0].shape[1] // 2
    width = half - occ_count
    points = point_sets[0].shape[0]
    step = 768 if width % 768 == 0 else width
    per = width // step
    total = 2 * n * rows

    def body(*refs):
        ins, w_ref = refs[:n], refs[n]
        sets = refs[n + 1 : n + 5]
        out, stacked = refs[n + 5 :]
        i = pl.program_id(0)

        @pl.when(i == 0)
        def _():
            out[...] = jnp.zeros_like(out)

        for s in range(2):

            @pl.when(i // per == s)
            def _(s=s):
                k = pl.multiple_of((i - s * per) * step, 128)
                w = w_ref[:, pl.ds(s * width + k, step)]
                for j in range(n):
                    x = ins[j][:, pl.ds(s * half + occ_count + k, step)]
                    for t in range(2):
                        at = (t * n + j) * rows
                        high, low = parts(x * w[t : t + 1])
                        stacked[pl.ds(at, rows), :] = high
                        stacked[pl.ds(total + at, rows), :] = low
                out[...] += contract_parts(stacked[...], sets[2 * s][...], sets[2 * s + 1][...])

    whole = lambda a: pl.BlockSpec(a.shape, lambda i: (0, 0))
    return pl.pallas_call(
        body,
        grid=(2 * per,),
        in_specs=[whole(b) for b in blocks]
        + [whole(weight)]
        + [
            pl.BlockSpec((points, step), lambda i: (0, jnp.minimum(i, per - 1))),
            pl.BlockSpec((points, step), lambda i: (0, jnp.minimum(i, per - 1))),
            pl.BlockSpec((points, step), lambda i: (0, jnp.maximum(i - per, 0))),
            pl.BlockSpec((points, step), lambda i: (0, jnp.maximum(i - per, 0))),
        ],
        out_specs=pl.BlockSpec((total, points), lambda i: (0, 0)),
        out_shape=jax.ShapeDtypeStruct((total, points), jnp.float32),
        scratch_shapes=[pltpu.VMEM((2 * total, step), jnp.bfloat16)],
        compiler_params=limit(24),
        cost_estimate=pl.CostEstimate(
            flops=6 * total * points * 2 * width, bytes_accessed=14_000_000, transcendentals=0
        ),
        name="vir_greens",
    )(*blocks, weight, *point_sets)


def occ_greens(here, there, point_sets):
    columns = here.shape[0] - 8
    width = here.shape[1]
    points, count = point_sets[0].shape

    def body(here_ref, there_ref, *refs):
        sets, (out, stacked) = refs[:4], refs[4:]
        total = None
        for chip, ref in enumerate((here_ref, there_ref)):
            energy = ref[pl.ds(columns, 1), :]
            for t in range(2):
                x = ref[pl.ds(0, columns), :] * jnp.exp(IMAG_TIMES[t] * energy)
                high, low = parts(x)
                k = pl.ds(chip * width, width)
                stacked[pl.ds(t * columns, columns), k] = high
                stacked[pl.ds((2 + t) * columns, columns), k] = low
        for i in range(4):
            part = contract_parts(stacked[:, pl.ds(i * count, count)], *parts(sets[i][...]))
            total = part if total is None else total + part
        out[...] = total

    return pl.pallas_call(
        body,
        out_shape=jax.ShapeDtypeStruct((2 * columns, points), jnp.float32),
        scratch_shapes=[pltpu.VMEM((4 * columns, 2 * width), jnp.bfloat16)],
        compiler_params=limit(16),
        name="occ_greens",
    )(here, there, *point_sets)


def projections(vir_here, vir_there, occ, waves, own):
    rows, points = occ.shape
    count = waves.shape[0]
    step = 512
    blocks = rows // (2 * own * SIDE)
    share = rows // blocks
    inner = share // (2 * own)

    def body(a_ref, b_ref, o_ref, w_ref, *refs):
        outs, stacked = refs[:-1], refs[-1]

        @pl.when(pl.program_id(0) == 0)
        def _():
            response = -(o_ref[...] * (a_ref[...] + b_ref[...]))
            early, late = response[: rows // 2], response[rows // 2 :]
            spectral = [TABLE[k][0] * early + TABLE[k][1] * late for k in range(2)]
            for j in range(blocks * inner):
                both = jnp.concatenate([s[j * own : (j + 1) * own] for s in spectral], axis=0)
                high, low = parts(both)
                stacked[pl.ds(2 * own * j, 2 * own), :] = high
                stacked[pl.ds(rows + 2 * own * j, 2 * own), :] = low

        result = contract_parts(stacked[...], *parts(w_ref[...]))
        for d in range(blocks):
            outs[d][...] = result[d * share : (d + 1) * share]

    whole = pl.BlockSpec((rows, points), lambda i: (0, 0))
    return pl.pallas_call(
        body,
        grid=(count // step,),
        in_specs=[whole] * 3 + [pl.BlockSpec((step, points), lambda i: (i, 0))],
        out_specs=[pl.BlockSpec((share, step), lambda i: (0, i))] * blocks,
        out_shape=[jax.ShapeDtypeStruct((share, count), jnp.float32)] * blocks,
        scratch_shapes=[pltpu.VMEM((2 * rows, points), jnp.bfloat16)],
        compiler_params=limit(24),
        cost_estimate=pl.CostEstimate(
            flops=6 * rows * points * count, bytes_accessed=8_000_000, transcendentals=0
        ),
        name="projections",
    )(vir_here, vir_there, occ, waves)


def summed_blocks(arrays):
    rows, waves = arrays[0].shape
    step = 1024
    share = rows // SIDE

    def body(*refs):
        total = refs[0][...]
        for r in refs[1:SIDE]:
            total = total + r[...]
        for d in range(SIDE):
            refs[SIDE + d][...] = total[d * share : (d + 1) * share]

    return pl.pallas_call(
        body,
        grid=(waves // step,),
        in_specs=[pl.BlockSpec((rows, step), lambda i: (0, i))] * SIDE,
        out_specs=[pl.BlockSpec((share, step), lambda i: (0, i))] * SIDE,
        out_shape=[jax.ShapeDtypeStruct((share, waves), jnp.float32)] * SIDE,
        compiler_params=limit(12),
        cost_estimate=pl.CostEstimate(
            flops=3 * rows * waves, bytes_accessed=20 * rows * waves, transcendentals=0
        ),
        name="summed_blocks",
    )(*arrays)


def after(x, event):
    return lax.optimization_barrier((x, event))[0]


def on_device(occ_points, vir_points, occ_cols, vir_cols, occ_energy, vir_energy, plane_waves):
    _, occ_count = occ_points.shape
    own = occ_cols.shape[0]
    moments = jnp.array(IMAG_TIMES, jnp.float32)

    cols = joined([occ_cols, vir_cols], 1)
    block = [from_owner(cols, 0, other) for other in (False, True)]
    block = joined(block, 1)
    block = joined([block] + [inner_shift(block, -d) for d in range(1, SIDE)], 0)
    blocks = [block] + [None] * (SIDE - 1)
    for d in (1, 3, 2):
        if d == 2:
            block = after(block, (blocks[1], blocks[3]))
        blocks[d] = outer_shift(block, -d)

    energy = jnp.concatenate([occ_energy, vir_energy])
    energy_other = swap(energy, "core")
    vir_both = jnp.concatenate([vir_energy, energy_other[occ_count:]])
    vir_weight = jnp.exp(-moments[:, None] * vir_both[None, :])
    occ_chip = jnp.concatenate([occ_energy, energy_other[:occ_count]])
    occ_chip = jnp.broadcast_to(occ_chip[None], (8, 2 * occ_count))
    occ_points_there = swap(occ_points, "yl")
    vir_sets = list(split(vir_points))
    vir_other = swap(vir_points, "core")
    vir_sets += list(split(vir_other))
    occ_near = after(occ_points, (blocks[1], blocks[3]))
    occ_sets = [occ_near, swap(occ_near, "core")]

    sums = [[None] * SIDE for _ in range(2)]
    for n, group in enumerate(((1, 3), (0, 2))):
        pair = [blocks[d] for d in group]
        occ_here = picked(pair, occ_chip, occ_count, cols.shape[1])
        occ_there = swap(occ_here, "yl")
        vir_here = vir_greens(pair, vir_weight, vir_sets, occ_count)
        vir_there = swap(vir_here, "yl")
        if n == 0:
            occ_far, waves = after((occ_points_there, plane_waves), vir_here)
            occ_sets += [occ_far, swap(occ_far, "core")]
            wave_sets = (plane_waves, swap(waves, "core"))
        occ_green = occ_greens(occ_here, occ_there, occ_sets)
        for s in range(2):
            found = projections(vir_here, vir_there, occ_green, wave_sets[s], own)
            for j, d in enumerate(group):
                sums[s][d] = outer_shift(found[j], d) if d else found[j]

    results = []
    for s, other in enumerate((False, True)):
        finished = summed_blocks(sums[s])
        for d in range(SIDE):
            results.append(to_owner(finished[d], d, other))
    total = sum(results[1:], results[0])
    return jnp.transpose(total.reshape(2, own, -1), (0, 2, 1))


def solution(mesh):
    split = Mesh(mesh.devices.reshape(SIDE, 2, SIDE, 2, 2), PTS + ORB)
    in_specs = (
        P(PTS, ORB),
        P(PTS, ORB),
        P(PTS, ORB),
        P(PTS, ORB),
        P(ORB),
        P(ORB),
        P(ORB, PTS),
    )
    out_specs = P(None, ORB, PTS)
    return jax.shard_map(
        on_device, mesh=split, in_specs=in_specs, out_specs=out_specs, check_vma=False
    )
```

```python
import math

import jax
import jax.numpy as jnp
from jax import lax
from jax.experimental import pallas as pl
from jax.experimental.pallas import tpu as pltpu
from jax.sharding import Mesh
from jax.sharding import PartitionSpec as P

PTS = ("z", "yh", "x")
ORB = ("yl", "core")
SIDE = 4

IMAG_TIMES = (0.3, 1.2)
FREQUENCIES = (0.5, 2.0)
QUAD_WEIGHTS = (0.6, 1.8)
TABLE = [[2.0 * q * math.cos(w * t) for q, t in zip(QUAD_WEIGHTS, IMAG_TIMES)] for w in FREQUENCIES]

MIB = 1024 * 1024


def limit(mib):
    return pltpu.CompilerParams(vmem_limit_bytes=mib * MIB)


def swap(x, axis):
    return lax.ppermute(x, axis, [(0, 1), (1, 0)])


def outer_shift(x, by):
    pairs = []
    for z in range(SIDE):
        for k in range(SIDE):
            for core in range(2):
                to = (z, (k + by) % SIDE) if core else ((z + by) % SIDE, k)
                pairs.append(((z * SIDE + k) * 2 + core, (to[0] * SIDE + to[1]) * 2 + core))
    return lax.ppermute(x, ("z", "x", "core"), pairs)


def inner_shift(x, by):
    pairs = []
    for z in range(SIDE):
        for k in range(SIDE):
            for core in range(2):
                to = ((z + by) % SIDE, k) if core else (z, (k + by) % SIDE)
                pairs.append(((z * SIDE + k) * 2 + core, (to[0] * SIDE + to[1]) * 2 + core))
    return lax.ppermute(x, ("z", "x", "core"), pairs)


def inner_pairs(by, other):
    place = lambda z, y, x, c: (((z % SIDE) * 2 + y) * SIDE + x % SIDE) * 2 + c
    pairs = []
    for z in range(SIDE):
        for y in range(2):
            for x in range(SIDE):
                near = place(z, y, x + by, 1 if other else 0)
                far = place(z + by, 1 - y, x, 0 if other else 1)
                pairs += [(place(z, y, x, 0), near), (place(z, y, x, 1), far)]
    return pairs


def to_owner(x, by, other):
    return lax.ppermute(x, PTS + ("core",), inner_pairs(by, other))


def from_owner(x, by, other):
    pairs = [(b, a) for a, b in inner_pairs(by, other)]
    return lax.ppermute(x, PTS + ("core",), pairs)


def joined(blocks, axis):
    shape = list(blocks[0].shape)
    shape[axis] = sum(b.shape[axis] for b in blocks)

    def body(*refs):
        start = 0
        for r in refs[:-1]:
            at = pl.ds(start, r.shape[axis])
            if axis:
                refs[-1][:, at] = r[...]
            else:
                refs[-1][at, :] = r[...]
            start += r.shape[axis]

    return pl.pallas_call(
        body,
        out_shape=jax.ShapeDtypeStruct(tuple(shape), blocks[0].dtype),
        compiler_params=limit(6),
        name="joined",
    )(*blocks)


def picked(blocks, energy, occ_count, core_width):
    rows = blocks[0].shape[0]
    n = len(blocks)

    def body(*refs):
        ins, last, out = refs[: 2 * n], refs[2 * n], refs[2 * n + 1]
        for i in range(n):
            for s in range(2):
                at = (pl.ds(i * rows, rows), pl.ds(s * occ_count, occ_count))
                out[at] = ins[2 * i + s][...]
        out[pl.ds(n * rows, 8), :] = last[...]

    def slot(s):
        at = s * core_width // occ_count
        return pl.BlockSpec((rows, occ_count), lambda i: (0, at))

    return pl.pallas_call(
        body,
        grid=(1,),
        in_specs=[slot(s) for _ in range(n) for s in range(2)]
        + [pl.BlockSpec(energy.shape, lambda i: (0, 0))],
        out_specs=pl.BlockSpec((n * rows + 8, 2 * occ_count), lambda i: (0, 0)),
        out_shape=jax.ShapeDtypeStruct((n * rows + 8, 2 * occ_count), blocks[0].dtype),
        compiler_params=limit(4),
        name="picked",
    )(*[b for b in blocks for _ in range(2)], energy)


def parts(x):
    high = x.astype(jnp.bfloat16)
    return high, (x - high.astype(jnp.float32)).astype(jnp.bfloat16)


def contract(left, right):
    return lax.dot_general(
        left, right, (((1,), (1,)), ((), ())), preferred_element_type=jnp.float32
    )


def split(x):
    rows, width = x.shape
    step = 768 if width % 768 == 0 else width

    def body(ref, high, low):
        high[...], low[...] = parts(ref[...])

    spec = pl.BlockSpec((rows, step), lambda i: (0, i))
    return pl.pallas_call(
        body,
        grid=(width // step,),
        in_specs=[spec],
        out_specs=[spec] * 2,
        out_shape=[jax.ShapeDtypeStruct(x.shape, jnp.bfloat16)] * 2,
        compiler_params=limit(12),
        name="split",
    )(x)


def contract_parts(stacked, high, low):
    rows = stacked.shape[0] // 2
    both = contract(stacked, high)
    return (both[:rows] + both[rows:]) + contract(stacked[:rows], low)


def vir_greens(blocks, weight, point_sets, occ_count):
    n = len(blocks)
    rows = blocks[0].shape[0]
    half = blocks[0].shape[1] // 2
    width = half - occ_count
    points = point_sets[0].shape[0]
    step = 768 if width % 768 == 0 else width
    per = width // step
    total = 2 * n * rows

    def body(*refs):
        ins, w_ref = refs[:n], refs[n]
        sets = refs[n + 1 : n + 5]
        out, stacked = refs[n + 5 :]
        found = None
        for i in range(2 * per):
            s, k = i // per, (i % per) * step
            for j in range(n):
                x = ins[j][:, pl.ds(s * half + occ_count + k, step)]
                for t in range(2):
                    at = (t * n + j) * rows
                    high, low = parts(x * w_ref[pl.ds(t, 1), pl.ds(s * width + k, step)])
                    stacked[i % 2, pl.ds(at, rows), :] = high
                    stacked[i % 2, pl.ds(total + at, rows), :] = low
            right = [sets[2 * s + p][:, pl.ds(k, step)] for p in range(2)]
            part = contract_parts(stacked[i % 2], *right)
            found = part if found is None else found + part
        out[...] = found

    return pl.pallas_call(
        body,
        out_shape=jax.ShapeDtypeStruct((total, points), jnp.float32),
        scratch_shapes=[pltpu.VMEM((2, 2 * total, step), jnp.bfloat16)],
        compiler_params=limit(24),
        cost_estimate=pl.CostEstimate(
            flops=6 * total * points * 2 * width, bytes_accessed=14_000_000, transcendentals=0
        ),
        name="vir_greens",
    )(*blocks, weight, *point_sets)


def occ_greens(here, there, point_sets):
    columns = here.shape[0] - 8
    width = here.shape[1]
    points, count = point_sets[0].shape

    def body(here_ref, there_ref, *refs):
        sets, (out, stacked) = refs[:4], refs[4:]
        total = None
        for chip, ref in enumerate((here_ref, there_ref)):
            energy = ref[pl.ds(columns, 1), :]
            for t in range(2):
                x = ref[pl.ds(0, columns), :] * jnp.exp(IMAG_TIMES[t] * energy)
                high, low = parts(x)
                k = pl.ds(chip * width, width)
                stacked[pl.ds(t * columns, columns), k] = high
                stacked[pl.ds((2 + t) * columns, columns), k] = low
        for i in range(4):
            part = contract_parts(stacked[:, pl.ds(i * count, count)], *parts(sets[i][...]))
            total = part if total is None else total + part
        out[...] = total

    return pl.pallas_call(
        body,
        out_shape=jax.ShapeDtypeStruct((2 * columns, points), jnp.float32),
        scratch_shapes=[pltpu.VMEM((4 * columns, 2 * width), jnp.bfloat16)],
        compiler_params=limit(16),
        name="occ_greens",
    )(here, there, *point_sets)


def projections(vir_here, vir_there, occ, waves, own):
    rows, points = occ.shape
    count = waves.shape[0]
    step = 512
    blocks = rows // (2 * own * SIDE)
    share = rows // blocks
    inner = share // (2 * own)

    def body(a_ref, b_ref, o_ref, w_ref, *refs):
        outs, stacked = refs[:-1], refs[-1]

        @pl.when(pl.program_id(0) == 0)
        def _():
            response = -(o_ref[...] * (a_ref[...] + b_ref[...]))
            early, late = response[: rows // 2], response[rows // 2 :]
            spectral = [TABLE[k][0] * early + TABLE[k][1] * late for k in range(2)]
            for j in range(blocks * inner):
                both = jnp.concatenate([s[j * own : (j + 1) * own] for s in spectral], axis=0)
                high, low = parts(both)
                stacked[pl.ds(2 * own * j, 2 * own), :] = high
                stacked[pl.ds(rows + 2 * own * j, 2 * own), :] = low

        result = contract_parts(stacked[...], *parts(w_ref[...]))
        for d in range(blocks):
            outs[d][...] = result[d * share : (d + 1) * share]

    whole = pl.BlockSpec((rows, points), lambda i: (0, 0))
    return pl.pallas_call(
        body,
        grid=(count // step,),
        in_specs=[whole] * 3 + [pl.BlockSpec((step, points), lambda i: (i, 0))],
        out_specs=[pl.BlockSpec((share, step), lambda i: (0, i))] * blocks,
        out_shape=[jax.ShapeDtypeStruct((share, count), jnp.float32)] * blocks,
        scratch_shapes=[pltpu.VMEM((2 * rows, points), jnp.bfloat16)],
        compiler_params=limit(24),
        cost_estimate=pl.CostEstimate(
            flops=6 * rows * points * count, bytes_accessed=8_000_000, transcendentals=0
        ),
        name="projections",
    )(vir_here, vir_there, occ, waves)


def summed_blocks(arrays):
    rows, waves = arrays[0].shape
    step = 1024
    share = rows // SIDE

    def body(*refs):
        total = refs[0][...]
        for r in refs[1:SIDE]:
            total = total + r[...]
        for d in range(SIDE):
            refs[SIDE + d][...] = total[d * share : (d + 1) * share]

    return pl.pallas_call(
        body,
        grid=(waves // step,),
        in_specs=[pl.BlockSpec((rows, step), lambda i: (0, i))] * SIDE,
        out_specs=[pl.BlockSpec((share, step), lambda i: (0, i))] * SIDE,
        out_shape=[jax.ShapeDtypeStruct((share, waves), jnp.float32)] * SIDE,
        compiler_params=limit(12),
        cost_estimate=pl.CostEstimate(
            flops=3 * rows * waves, bytes_accessed=20 * rows * waves, transcendentals=0
        ),
        name="summed_blocks",
    )(*arrays)


def after(x, event):
    return lax.optimization_barrier((x, event))[0]


def on_device(occ_points, vir_points, occ_cols, vir_cols, occ_energy, vir_energy, plane_waves):
    _, occ_count = occ_points.shape
    own = occ_cols.shape[0]
    moments = jnp.array(IMAG_TIMES, jnp.float32)

    cols = joined([occ_cols, vir_cols], 1)
    block = [from_owner(cols, 0, other) for other in (False, True)]
    block = joined(block, 1)
    block = joined([block] + [inner_shift(block, -d) for d in range(1, SIDE)], 0)
    blocks = [block] + [None] * (SIDE - 1)
    for d in (1, 3, 2):
        if d == 2:
            block = after(block, (blocks[1], blocks[3]))
        blocks[d] = outer_shift(block, -d)

    energy = jnp.concatenate([occ_energy, vir_energy])
    energy_other = swap(energy, "core")
    vir_both = jnp.concatenate([vir_energy, energy_other[occ_count:]])
    vir_weight = jnp.exp(-moments[:, None] * vir_both[None, :])
    occ_chip = jnp.concatenate([occ_energy, energy_other[:occ_count]])
    occ_chip = jnp.broadcast_to(occ_chip[None], (8, 2 * occ_count))
    occ_points_there = swap(occ_points, "yl")
    vir_sets = list(split(vir_points))
    vir_other = swap(vir_points, "core")
    vir_sets += list(split(vir_other))
    occ_near = after(occ_points, (blocks[1], blocks[3]))
    occ_sets = [occ_near, swap(occ_near, "core")]

    sums = [[None] * SIDE for _ in range(2)]
    for n, group in enumerate(((1, 3), (0, 2))):
        pair = [blocks[d] for d in group]
        occ_here = picked(pair, occ_chip, occ_count, cols.shape[1])
        occ_there = swap(occ_here, "yl")
        vir_here = vir_greens(pair, vir_weight, vir_sets, occ_count)
        vir_there = swap(vir_here, "yl")
        if n == 0:
            occ_far, waves = after((occ_points_there, plane_waves), vir_here)
            occ_sets += [occ_far, swap(occ_far, "core")]
            wave_sets = (plane_waves, swap(waves, "core"))
        occ_green = occ_greens(occ_here, occ_there, occ_sets)
        for s in range(2):
            found = projections(vir_here, vir_there, occ_green, wave_sets[s], own)
            for j, d in enumerate(group):
                sums[s][d] = outer_shift(found[j], d) if d else found[j]

    results = []
    for s, other in enumerate((False, True)):
        finished = summed_blocks(sums[s])
        for d in range(SIDE):
            results.append(to_owner(finished[d], d, other))
    total = sum(results[1:], results[0])
    return jnp.transpose(total.reshape(2, own, -1), (0, 2, 1))


def solution(mesh):
    split = Mesh(mesh.devices.reshape(SIDE, 2, SIDE, 2, 2), PTS + ORB)
    in_specs = (
        P(PTS, ORB),
        P(PTS, ORB),
        P(PTS, ORB),
        P(PTS, ORB),
        P(ORB),
        P(ORB),
        P(ORB, PTS),
    )
    out_specs = P(None, ORB, PTS)
    return jax.shard_map(
        on_device, mesh=split, in_specs=in_specs, out_specs=out_specs, check_vma=False
    )
```
